32 devices in a mesh: seq: 4 (over y, x), rep: 8 (over z, core).
Axes of the slice: x: 2, y: 2, z: 4, core: 2. Of those that a mesh axis runs over, the one named last changes fastest.
Arguments:
- tile_embed: bfloat16 [8, 4096, 768], P('rep', 'seq'), may hold values from -6 to 6
- tile_source: int32 [8, 4096], P('rep', 'seq'), may hold values from 0 to 4095, as said below
- slide_len: int32 [8], P('rep'), may hold values from 2048 to 4096
- grad_out: bfloat16 [8, 4096, 768], P('rep', 'seq'), may hold values from -6 to 6
- w_query: bfloat16 [768, 768], replicated, may hold values from -0.11727427342914273 to 0.11727427342914273
- w_key: bfloat16 [768, 768], replicated, may hold values from -0.11727427342914273 to 0.11727427342914273
- w_value: bfloat16 [768, 768], replicated, may hold values from -0.21875 to 0.21875
- w_out: bfloat16 [768, 768], replicated, may hold values from -0.21875 to 0.21875
Outputs:
- encoded: bfloat16 [8, 4096, 768], P('rep', 'seq')
- embed_grad: bfloat16 [8, 4096, 768], P('rep', 'seq')
- grad_query: float32 [768, 768], replicated
- grad_key: float32 [768, 768], replicated
- grad_value: float32 [768, 768], replicated
- grad_outproj: float32 [768, 768], replicated
The draws below stay inside these ranges and needn't reach their ends.
Inputs may be any that keep to these rules, and one draw needn't show every extreme that they name: For each slide, tile_source is a permutation of 0 to 4095; each run of 1024 slide positions (aligned) takes exactly 1024 // (number of such runs) rows from each aligned run of 1024 rows of tile_embed.
All inputs are finite; a program needn't handle non-finite values.
Results may differ from the reference program's by a relative error of at most 0.0025.
The reference program's roundings to bfloat16 on the way count: a program that leaves them out, or rounds other values in their place, can miss the bound.
Values may be sent and summed in bfloat16 or wider, within the bound.
No kernel may reach another device: no remote copies, remote signals or barrier semaphores. Data moves between devices by JAX's collectives and lax.ppermute only.
A program may use at most 192 MiB of HBM per device.

```python
import jax
import jax.numpy as jnp
from jax import lax

D = 768
HEADS = 16
SEG = 1024
RATE = 16
TOK_DEV = 1024
SLIDE = 4096
SLIDES = 8


def slide_order(key):
    owners = SLIDE // TOK_DEV
    portion = TOK_DEV // owners
    first_key, second_key = jax.random.split(key)
    mixed = jax.vmap(lambda subkey: jax.random.permutation(subkey, TOK_DEV))(jax.random.split(first_key, owners))
    placed = mixed + (jnp.arange(owners) * TOK_DEV)[:, None]
    placed = placed.reshape(owners, owners, portion).transpose(1, 0, 2).reshape(owners, TOK_DEV)
    shuffle = jax.vmap(lambda subkey: jax.random.permutation(subkey, TOK_DEV))(jax.random.split(second_key, owners))
    placed = jnp.take_along_axis(placed, shuffle, axis=1)
    return placed.reshape(SLIDE).astype(jnp.int32)


def draw_tile_source(key, part):
    return jax.vmap(slide_order)(jax.random.split(jax.random.fold_in(key, 7), SLIDES))


def plant_basis(key):
    basis_key = jax.random.fold_in(key, 11)
    sign_key, half_key, head_key, column_key = jax.random.split(basis_key, 4)
    first_sign = (2 * jax.random.randint(sign_key, (D,), 0, 2) - 1).astype(jnp.float32)
    halves = jnp.where(jax.random.permutation(half_key, D) < D // 2, 1.0, -1.0).astype(jnp.float32)
    second_sign = first_sign * halves
    head_width = D // HEADS
    column_sign = (2 * jax.random.randint(column_key, (head_width,), 0, 2) - 1).astype(jnp.float32)
    chosen_head = jax.random.randint(head_key, (), 0, HEADS)
    return (first_sign, second_sign, halves, column_sign, chosen_head)


def planted_weight(key, salt):
    first_sign, second_sign, halves, column_sign, chosen_head = plant_basis(key)
    head_width = D // HEADS
    noise_key = jax.random.fold_in(key, salt)
    noise = jax.random.truncated_normal(noise_key, -3.0, 3.0, (D, D), jnp.float32)
    noise = noise * D ** (-0.5)
    along_first = jnp.dot(first_sign, noise, precision=lax.Precision.HIGHEST) / D
    along_second = jnp.dot(second_sign, noise, precision=lax.Precision.HIGHEST) / D
    cleaned = noise - first_sign[:, None] * along_first[None, :] - second_sign[:, None] * along_second[None, :]
    columns = jnp.arange(D)
    in_head = columns // head_width == chosen_head
    strength = (16.0 / head_width ** 0.5) ** 0.5
    planted = cleaned + strength / D * first_sign[:, None] * column_sign[columns % head_width][None, :]
    weight = jnp.where(in_head[None, :], planted, noise)
    limit = 3.25 * D ** (-0.5)
    return jnp.clip(weight, -limit, limit).astype(jnp.bfloat16)


def draw_w_query(key, part):
    return planted_weight(key, 21)


def draw_w_key(key, part):
    return planted_weight(key, 22)


def draw_tile_embed(key, part):
    first_sign, second_sign, halves, column_sign, chosen_head = plant_basis(key)
    sources = draw_tile_source(key, part)
    noise_key = jax.random.fold_in(key, 31)
    rows = jax.random.truncated_normal(noise_key, -6.0, 6.0, (SLIDES, SLIDE, D), jnp.float32)
    spots = chosen_head % RATE + RATE * jnp.arange(4)
    level_key, sign_key = jax.random.split(jax.random.fold_in(key, 41))
    levels = jnp.array([1.0, 1.5, 2.0, 2.5, 3.0], jnp.float32)
    picked = levels[jax.random.randint(level_key, (SLIDES, 2), 0, 5)]
    signs = (2 * jax.random.randint(sign_key, (SLIDES, 2), 0, 2) - 1).astype(jnp.float32)
    leading = jnp.broadcast_to(jnp.array([4.0, 3.96875], jnp.float32)[None, :], (SLIDES, 2))
    leading_offsets = jnp.broadcast_to(jnp.array([2.0, -2.0], jnp.float32)[None, :], (SLIDES, 2))
    strengths = jnp.concatenate([leading, picked], axis=1)
    offsets = jnp.concatenate([leading_offsets, signs], axis=1)
    planted = first_sign[None, None, :] * (strengths[..., None] + offsets[..., None] * halves[None, None, :])
    targets = sources[:, spots].astype(jnp.int32)
    slide_index = jnp.broadcast_to(jnp.arange(SLIDES)[:, None], targets.shape).astype(jnp.int32)
    rows = rows.at[slide_index, targets].set(planted)
    return rows.astype(jnp.bfloat16)


def place_ends(values, stream_key, low, largest):
    index_at = [jax.random.randint(jax.random.fold_in(stream_key, axis), (), 0, length) for axis, length in enumerate(values.shape)]
    longest = values.shape.index(max(values.shape))
    beside = index_at[:longest] + [(index_at[longest] + 1) % values.shape[longest]] + index_at[longest + 1:]
    return values.at[tuple(index_at)].set(low).at[tuple(beside)].set(largest)


def level_of(key, shape, cuts, low, largest):
    level = 1.0
    for dim, shards_of in cuts:
        steps = jax.random.uniform(jax.random.fold_in(jax.random.fold_in(key, 6), dim), (shards_of,), jnp.float32, low / len(cuts), largest / len(cuts))
        level = level * jnp.repeat(jnp.exp(steps), shape[dim] // shards_of).reshape((-1,) + (1,) * (len(shape) - 1 - dim))
    return level


def centred(own_key, extent, scale, reach, cuts=(), held_as=jnp.bfloat16):
    result = scale * jax.random.normal(own_key, extent, jnp.float32)
    if cuts:
        result = result * level_of(own_key, extent, cuts, -0.22, 0.18)
    return jnp.clip(result, -reach, reach).astype(held_as)


def setup_inputs(seed: int = 0) -> dict:
    arg_keys = jax.random.split(jax.random.key(seed), 9)
    tile_embed = draw_tile_embed(jax.random.fold_in(arg_keys[8], 71), 0)
    tile_source = draw_tile_source(jax.random.fold_in(arg_keys[8], 71), 0)
    slide_len = place_ends(jax.random.randint(arg_keys[2], (SLIDES,), SLIDE // 2, SLIDE + 1), jax.random.fold_in(arg_keys[2], 1), SLIDE // 2, SLIDE).astype(jnp.int32)
    grad_out = centred(arg_keys[3], (SLIDES, SLIDE, D), 1.0, 6.0, ((0, 8), (1, 4)))
    w_query = draw_w_query(jax.random.fold_in(arg_keys[8], 71), 0)
    w_key = draw_w_key(jax.random.fold_in(arg_keys[8], 71), 0)
    w_value = centred(arg_keys[6], (D, D), D ** -0.5, 0.21875)
    w_out = centred(arg_keys[7], (D, D), D ** -0.5, 0.21875)
    return dict(tile_embed=tile_embed, tile_source=tile_source, slide_len=slide_len, grad_out=grad_out, w_query=w_query, w_key=w_key, w_value=w_value, w_out=w_out)


NEGATIVE = -1.0e30


def chosen(dilation, head_count):
    return jnp.arange(dilation)[:, None] == (jnp.arange(head_count) % dilation)[None, :]


def sparse_rows(dense, dilation):
    row_count, head_count, trailing = dense.shape
    blocks = dense.astype(jnp.float32).reshape(row_count // dilation, dilation, head_count, trailing)
    selected = chosen(dilation, head_count)[None, :, :, None]
    return jnp.sum(jnp.where(selected, blocks, jnp.float32(0.0)), axis=1)


def spread_rows(sparse, dilation, filler):
    row_count, head_count, trailing = sparse.shape
    selected = chosen(dilation, head_count)[None, :, :, None]
    spread = jnp.where(selected, sparse[:, None], jnp.float32(filler))
    return spread.reshape(row_count * dilation, head_count, trailing)


def product(pattern, left_side, right_side):
    return jnp.einsum(pattern, left_side.astype(jnp.float32), right_side.astype(jnp.float32))


def masked_scores(queries, key_rows, key_ok, pieces, scaling):
    scores = product('nqd,nkd->nqk', queries, key_rows) * scaling
    return jnp.where(key_ok.reshape(pieces, 1, -1), scores, NEGATIVE)


def head_forward(queries, key_rows, values, key_ok, pieces, scaling):
    head_width = queries.shape[-1]
    queries = queries.reshape(pieces, -1, head_width)
    key_rows = key_rows.reshape(pieces, -1, head_width)
    values = values.reshape(pieces, -1, head_width)
    scores = masked_scores(queries, key_rows, key_ok, pieces, scaling)
    maxima = jnp.max(scores, axis=-1)
    weights = jnp.exp(scores - maxima[..., None])
    totals = jnp.sum(weights, axis=-1)
    numerator = product('nqk,nkd->nqd', weights.astype(jnp.bfloat16), values)
    return numerator.reshape(-1, head_width), maxima.reshape(-1), totals.reshape(-1)


def head_backward(queries, key_rows, values, key_ok, log_total, upstream, deltas, pieces, scaling):
    head_width = queries.shape[-1]
    queries = queries.reshape(pieces, -1, head_width)
    key_rows = key_rows.reshape(pieces, -1, head_width)
    values = values.reshape(pieces, -1, head_width)
    upstream = upstream.reshape(pieces, -1, head_width)
    scores = masked_scores(queries, key_rows, key_ok, pieces, scaling)
    probabilities = jnp.exp(scores - log_total.reshape(pieces, -1, 1))
    value_grad = product('nqk,nqd->nkd', probabilities.astype(jnp.bfloat16), upstream)
    prob_grad = product('nqd,nkd->nqk', upstream, values)
    score_grad = (probabilities * (prob_grad - deltas.reshape(pieces, -1, 1))).astype(jnp.bfloat16)
    query_grad = product('nqk,nkd->nqd', score_grad, key_rows) * scaling
    key_grad = product('nqk,nqd->nkd', score_grad, queries) * scaling
    return query_grad.reshape(-1, head_width), key_grad.reshape(-1, head_width), value_grad.reshape(-1, head_width)


def heads_map(function, arrays, pieces, scaling):
    transposed = tuple(jnp.moveaxis(member, 1, 0) for member in arrays)
    results = lax.map(lambda members: function(*members, pieces, scaling), transposed)
    return tuple(jnp.moveaxis(member, 0, 1) for member in results)


def merge_parts(local_part, remote, dilation):
    numer_local, max_local, total_local = local_part
    numer_far = spread_rows(remote[0], dilation, 0.0)
    max_far = spread_rows(remote[1][..., None], dilation, NEGATIVE)[..., 0]
    total_far = spread_rows(remote[2][..., None], dilation, 0.0)[..., 0]
    highest = jnp.maximum(max_local, max_far)
    weight_local = jnp.exp(max_local - highest)
    weight_far = jnp.exp(max_far - highest)
    combined = total_local * weight_local + total_far * weight_far
    output = (numer_local * weight_local[..., None] + numer_far * weight_far[..., None]) / combined[..., None]
    return output, highest + jnp.log(combined)


def slide_pass(embedded, upstream_in, length, w_query, w_key, w_value, w_out):
    row_count, features = embedded.shape
    head_dim = features // HEADS
    scaling = head_dim ** -0.5
    valid_rows = jnp.arange(row_count) < length
    queries = jnp.dot(embedded, w_query, preferred_element_type=jnp.float32).astype(jnp.bfloat16).reshape(row_count, HEADS, head_dim)
    key_rows = jnp.dot(embedded, w_key, preferred_element_type=jnp.float32).astype(jnp.bfloat16).reshape(row_count, HEADS, head_dim)
    values = jnp.dot(embedded, w_value, preferred_element_type=jnp.float32).astype(jnp.bfloat16).reshape(row_count, HEADS, head_dim)
    local_ok = jnp.broadcast_to(valid_rows[:, None], (row_count, HEADS))
    local_part = heads_map(head_forward, (queries, key_rows, values, local_ok), row_count // SEG, scaling)
    sparse_q = sparse_rows(queries, RATE).astype(jnp.bfloat16)
    sparse_k = sparse_rows(key_rows, RATE).astype(jnp.bfloat16)
    sparse_v = sparse_rows(values, RATE).astype(jnp.bfloat16)
    sparse_pos = jnp.arange(row_count // RATE)[:, None] * RATE + (jnp.arange(HEADS) % RATE)[None, :]
    sparse_ok = sparse_pos < length
    remote = heads_map(head_forward, (sparse_q, sparse_k, sparse_v, sparse_ok), 1, scaling)
    output, log_total = merge_parts(local_part, remote, RATE)
    attended = (output * valid_rows[:, None, None]).astype(jnp.bfloat16).reshape(row_count, features)
    encoded = (embedded.astype(jnp.float32) + jnp.dot(attended, w_out, preferred_element_type=jnp.float32)).astype(jnp.bfloat16)
    upstream = (jnp.dot(upstream_in, w_out.T, preferred_element_type=jnp.float32) * valid_rows[:, None]).astype(jnp.bfloat16).reshape(row_count, HEADS, head_dim)
    deltas = jnp.sum(upstream.astype(jnp.float32) * output, axis=-1)
    grad_outproj = jnp.dot(attended.T, upstream_in, preferred_element_type=jnp.float32)
    local_grads = heads_map(head_backward, (queries, key_rows, values, local_ok, log_total, upstream, deltas), row_count // SEG, scaling)
    sparse_up = sparse_rows(upstream, RATE).astype(jnp.bfloat16)
    sparse_delta = sparse_rows(deltas[..., None], RATE)[..., 0]
    sparse_total = sparse_rows(log_total[..., None], RATE)[..., 0]
    remote_grads = heads_map(head_backward, (sparse_q, sparse_k, sparse_v, sparse_ok, sparse_total, sparse_up, sparse_delta), 1, scaling)
    query_grad = (local_grads[0] + spread_rows(remote_grads[0], RATE, 0.0)).astype(jnp.bfloat16).reshape(row_count, features)
    key_grad = (local_grads[1] + spread_rows(remote_grads[1], RATE, 0.0)).astype(jnp.bfloat16).reshape(row_count, features)
    value_grad = (local_grads[2] + spread_rows(remote_grads[2], RATE, 0.0)).astype(jnp.bfloat16).reshape(row_count, features)
    embed_grad = upstream_in.astype(jnp.float32) + jnp.dot(query_grad, w_query.T, preferred_element_type=jnp.float32)
    embed_grad = embed_grad + jnp.dot(key_grad, w_key.T, preferred_element_type=jnp.float32)
    embed_grad = (embed_grad + jnp.dot(value_grad, w_value.T, preferred_element_type=jnp.float32)).astype(jnp.bfloat16)
    gradients = (jnp.dot(embedded.T, query_grad, preferred_element_type=jnp.float32),
                 jnp.dot(embedded.T, key_grad, preferred_element_type=jnp.float32),
                 jnp.dot(embedded.T, value_grad, preferred_element_type=jnp.float32),
                 grad_outproj)
    return encoded, embed_grad, gradients


def reference(tile_embed, tile_source, slide_len, grad_out, w_query, w_key, w_value, w_out):
    def per_slide(members):
        owned_rows, source, length, upstream_in = members
        embedded = jnp.take(owned_rows, source.astype(jnp.int32), axis=0)
        return slide_pass(embedded, upstream_in, length, w_query, w_key, w_value, w_out)

    encoded, embed_grad, gradients = lax.map(per_slide, (tile_embed, tile_source, slide_len, grad_out))
    return (encoded, embed_grad, jnp.sum(gradients[0], axis=0), jnp.sum(gradients[1], axis=0),
            jnp.sum(gradients[2], axis=0), jnp.sum(gradients[3], axis=0))
```

```python
import functools
import math

import jax
import jax.numpy as jnp
from jax import lax
from jax.experimental import pallas as pl
from jax.experimental.pallas import tpu as pltpu
from jax.sharding import PartitionSpec as P

HEADS = 16
SEG = 1024
RATE = 16
NEGATIVE = -1e30
LOG2E = 1.4426950408889634
GROUPS = 2
CALL = 2
STEP_AT = (0, 1, 3)
QB = 256
LANES = 128
PAD = 16
F32 = jnp.float32
BF16 = jnp.bfloat16


def nn(a, b):
    return lax.dot_general(a, b, (((1,), (0,)), ((), ())), preferred_element_type=F32)


def nt(a, b):
    return lax.dot_general(a, b, (((1,), (1,)), ((), ())), preferred_element_type=F32)


def tn(a, b):
    return lax.dot_general(a, b, (((0,), (0,)), ((), ())), preferred_element_type=F32)


def params(grid_rank=1):
    return pltpu.CompilerParams(
        dimension_semantics=("arbitrary",) * grid_rank, vmem_limit_bytes=56 * 1024 * 1024
    )


def cost(flops, size, exps=0):
    return pl.CostEstimate(flops=int(flops), bytes_accessed=int(size), transcendentals=int(exps))


def stack_rows(top, bottom):
    return jnp.concatenate([top, bottom], axis=0)


def dilated_body(width, alpha, scaling, n_ref, q_ref, g_ref, k_ref, v_ref, k2_ref, v2_ref,
                 bias_ref, one_ref, o_ref, lse_ref, dq_ref, dk_ref, dv_ref):
    head = pl.program_id(0)
    tokens = k_ref.shape[1]
    far = k2_ref.shape[1]
    q = q_ref[...]
    g = g_ref[...]
    q_aug = stack_rows(q, one_ref[:, :LANES])
    k_aug = stack_rows(k_ref[...], bias_ref[...])
    s1 = tn(k_aug, q_aug)
    t1 = jnp.max(s1, axis=0, keepdims=True) * alpha
    e1 = jnp.exp2(s1 * alpha - t1)
    l1 = jnp.sum(e1, axis=0, keepdims=True)
    u1 = nn(v_ref[...], e1.astype(BF16))
    k2 = k2_ref[...]
    v2 = v2_ref[...]
    row = lax.broadcasted_iota(jnp.int32, (far, LANES), 0)
    pos = ((row // width) ^ n_ref[1]) * tokens + (row % width) * RATE + head % RATE
    s2 = jnp.where(pos < n_ref[0], tn(k2, q) * alpha, NEGATIVE)
    t2 = jnp.max(s2, axis=0, keepdims=True)
    e2 = jnp.exp2(s2 - t2)
    l2 = jnp.sum(e2, axis=0, keepdims=True)
    u2 = nn(v2, e2.astype(BF16))
    top = jnp.maximum(t1, t2)
    a1 = jnp.exp2(t1 - top)
    a2 = jnp.exp2(t2 - top)
    total = a1 * l1 + a2 * l2
    o = (a1 * u1 + a2 * u2) / total
    lse = top + jnp.log2(total)
    o_ref[...] = o
    lse_ref[0] = jnp.broadcast_to(lse, (8, LANES))
    delta = jnp.sum(g.astype(F32) * o, axis=0, keepdims=True)
    lane = lax.broadcasted_iota(jnp.int32, (1, LANES), 1)
    mine = lane // width == (head % RATE) % (LANES // width)
    keep = jnp.where(mine, 1.0, 0.0)
    p2 = jnp.exp2(s2 - lse) * keep
    ds2 = (p2 * (tn(v2, g) - delta)).astype(BF16)
    dv_ref[...] = nt(g, p2.astype(BF16))
    dq_ref[...] = nn(k2, ds2) * scaling
    dk_ref[...] = nt(q, ds2) * scaling


def dilated(n, qt, gt, kt, vt, k2, v2, bias, one, width, alpha, scaling):
    features, tokens = qt.shape
    hd = features // HEADS
    far = k2.shape[1]
    per = LANES // width
    lanes = lambda h: (h, (h % RATE) // per)
    rows = lambda h: (h, 0)
    fixed = lambda h: (0, 0)
    return pl.pallas_call(
        functools.partial(dilated_body, width, alpha, scaling),
        grid=(HEADS,),
        in_specs=[
            pl.BlockSpec(memory_space=pltpu.SMEM),
            pl.BlockSpec((hd, LANES), lanes),
            pl.BlockSpec((hd, LANES), lanes),
            pl.BlockSpec((hd, tokens), rows),
            pl.BlockSpec((hd, tokens), rows),
            pl.BlockSpec((hd, far), rows),
            pl.BlockSpec((hd, far), rows),
            pl.BlockSpec((PAD, tokens), fixed),
            pl.BlockSpec((PAD, tokens), fixed),
        ],
        out_specs=[
            pl.BlockSpec((hd, LANES), rows),
            pl.BlockSpec((1, 8, LANES), lambda h: (h, 0, 0)),
            pl.BlockSpec((hd, LANES), rows),
            pl.BlockSpec((hd, far), rows),
            pl.BlockSpec((hd, far), rows),
        ],
        out_shape=[
            jax.ShapeDtypeStruct((features, LANES), F32),
            jax.ShapeDtypeStruct((HEADS, 8, LANES), F32),
            jax.ShapeDtypeStruct((features, LANES), F32),
            jax.ShapeDtypeStruct((features, far), F32),
            jax.ShapeDtypeStruct((features, far), F32),
        ],
        compiler_params=params(),
        cost_estimate=cost(HEADS * 8 * tokens * LANES * 64, features * tokens * 6),
        name="dilated",
    )(n, qt, gt, kt, vt, k2, v2, bias, one)


def local_body(first, width, alpha, scaling, settled, kept, *refs):
    (q_ref, k_ref, v_ref, g_ref, bias_ref, one_ref, valid_ref, osp_ref, lsp_ref, dq2_ref,
     dk2_ref, dv2_ref) = refs[:12]
    att_ref, dq_ref, dk_ref, dv_ref, ksp_ref, vsp_ref = refs[12 + kept : 18 + kept]
    e_ref, o_ref, t_ref, lse_ref, p_ref, ds_ref, acc_ref = refs[18 + kept :]
    head = first + pl.program_id(0)
    hd, tokens = q_ref.shape
    k_aug = stack_rows(k_ref[...], bias_ref[...])
    for start in range(0, tokens, QB):
        cols = slice(start, start + QB)
        q_aug = stack_rows(q_ref[:, cols], one_ref[:, cols])
        s = tn(k_aug, q_aug)
        t = jnp.max(s, axis=0, keepdims=True) * alpha
        e = jnp.exp2(s * alpha - t)
        total = jnp.sum(e, axis=0, keepdims=True)
        e_ref[:, cols] = e
        u = nn(v_ref[...], e.astype(BF16))
        o_ref[:, cols] = u / total
        t_ref[:, cols] = jnp.broadcast_to(t, (8, QB))
        lse_ref[:, cols] = jnp.broadcast_to(t + jnp.log2(total), (8, QB))
    per = LANES // width
    base = pl.multiple_of(((head % RATE) // per) * LANES, LANES)
    spot = pl.ds(base, LANES)
    lane = lax.broadcasted_iota(jnp.int32, (1, LANES), 1)
    mine = lane // width == (head % RATE) % per
    o_ref[:, spot] = jnp.where(mine, osp_ref[...], o_ref[:, spot])
    lse_ref[:, spot] = jnp.where(mine, lsp_ref[0], lse_ref[:, spot])
    att_ref[...] = (o_ref[...] * valid_ref[0:1, :]).astype(BF16)
    for start in range(0, tokens, QB):
        cols = slice(start, start + QB)
        g = g_ref[:, cols]
        delta = jnp.sum(g.astype(F32) * o_ref[:, cols], axis=0, keepdims=True)
        factor = jnp.exp2(t_ref[0:1, cols] - lse_ref[0:1, cols])
        p = e_ref[:, cols] * factor
        p_ref[:, cols] = p.astype(BF16)
        ds_ref[:, cols] = (p * (tn(v_ref[...], g) - delta)).astype(BF16)
    acc_ref[...] = nn(k_ref[...], ds_ref[...]) * scaling
    acc_ref[:, spot] += dq2_ref[...]
    dq_ref[...] = acc_ref[...].astype(BF16)
    for weights, rows_in, extra, out, special, unit in (
        (ds_ref, q_ref, dk2_ref, dk_ref, ksp_ref, scaling),
        (p_ref, g_ref, dv2_ref, dv_ref, vsp_ref, None),
    ):
        total = nt(weights[...], rows_in[...]).T
        acc_ref[...] = total if unit is None else total * unit
        if settled:
            acc_ref[:, spot] += jnp.where(mine, extra[...], 0.0)
        out[...] = acc_ref[...].astype(BF16)
        special[...] = acc_ref[:, spot]


def local(group, size, first, count, prior, qt, kt, vt, gt, bias, one, valid, osp, lsp, dq2,
          dk2, dv2, settled, width, alpha, scaling):
    features, tokens = qt.shape
    hd = features // HEADS
    per = LANES // width
    rows = lambda h: (h + first, 0)
    mine = lambda h: (h + first - group, 0)
    fixed = lambda h: (0, 0)
    block = pl.BlockSpec((hd, tokens), rows)
    special = pl.BlockSpec((hd, LANES), rows)
    extra = special if settled else pl.BlockSpec((hd, LANES), fixed)
    kept = len(prior)
    return pl.pallas_call(
        functools.partial(local_body, first, width, alpha, scaling, settled, kept),
        grid=(count,),
        in_specs=[
            block, block, block, block,
            pl.BlockSpec((PAD, tokens), fixed),
            pl.BlockSpec((PAD, tokens), fixed),
            pl.BlockSpec((8, tokens), fixed),
            special,
            pl.BlockSpec((1, 8, LANES), lambda h: (h + first, 0, 0)),
            special, extra, extra,
        ] + [pl.BlockSpec(memory_space=pl.ANY)] * kept,
        out_specs=[pl.BlockSpec((hd, tokens), mine)] * 4 + [pl.BlockSpec((hd, LANES), mine)] * 2,
        out_shape=[jax.ShapeDtypeStruct((size * hd, tokens), BF16)] * 4
        + [jax.ShapeDtypeStruct((size * hd, LANES), F32)] * 2,
        scratch_shapes=[
            pltpu.VMEM((tokens, tokens), F32),
            pltpu.VMEM((hd, tokens), F32),
            pltpu.VMEM((8, tokens), F32),
            pltpu.VMEM((8, tokens), F32),
            pltpu.VMEM((tokens, tokens), BF16),
            pltpu.VMEM((tokens, tokens), BF16),
            pltpu.VMEM((hd, tokens), F32),
        ],
        input_output_aliases={12 + i: i for i in range(kept)},
        compiler_params=params(),
        cost_estimate=cost(count * 8 * tokens * tokens * 256, count * hd * tokens * 16),
        name="local%d" % first,
    )(qt, kt, vt, gt, bias, one, valid, osp, lsp, dq2, dk2, dv2, *prior)


def settle_body(first, width, k_ref, v_ref, dk2_ref, dv2_ref, _, __, k_out, v_out):
    head = first + pl.program_id(0)
    lane = lax.broadcasted_iota(jnp.int32, (1, LANES), 1)
    mine = lane // width == (head % RATE) % (LANES // width)
    k_out[...] = (k_ref[...] + jnp.where(mine, dk2_ref[...], 0.0)).astype(BF16)
    v_out[...] = (v_ref[...] + jnp.where(mine, dv2_ref[...], 0.0)).astype(BF16)


def settle(first, dk, dv, ksp, vsp, dk2, dv2, width):
    rows_all = dk.shape[0]
    hd = dk2.shape[0] // HEADS
    per = LANES // width
    mine = pl.BlockSpec((hd, LANES), lambda h: (h, 0))
    rows = pl.BlockSpec((hd, LANES), lambda h: (h + first, 0))
    spot = pl.BlockSpec((hd, LANES), lambda h: (h, ((h + first) % RATE) // per))
    whole = pl.BlockSpec(memory_space=pl.ANY)
    return pl.pallas_call(
        functools.partial(settle_body, first, width),
        grid=(rows_all // hd,),
        in_specs=[mine, mine, rows, rows, whole, whole],
        out_specs=[spot, spot],
        out_shape=[jax.ShapeDtypeStruct(dk.shape, BF16)] * 2,
        input_output_aliases={4: 0, 5: 1},
        compiler_params=params(),
        cost_estimate=cost(rows_all * LANES * 4, rows_all * LANES * 24),
        name="settle%d" % first,
    )(ksp, vsp, dk2, dv2, dk, dv)


def pick_body(index_ref, rows_ref, out_ref, hot_ref):
    @pl.when(pl.program_id(0) == 0)
    def _():
        which = lax.broadcasted_iota(jnp.int32, hot_ref.shape, 1) == index_ref[...]
        hot_ref[...] = jnp.where(which, 1.0, 0.0).astype(BF16)

    out_ref[...] = nn(hot_ref[...], rows_ref[...]).astype(BF16)


def pick(index, rows, name):
    total, features = rows.shape
    count = index.shape[0]
    block = 2 * LANES if features % (2 * LANES) == 0 else features
    return pl.pallas_call(
        pick_body,
        grid=(features // block,),
        in_specs=[
            pl.BlockSpec((count, 1), lambda i: (0, 0)),
            pl.BlockSpec((total, block), lambda i: (0, i)),
        ],
        out_specs=pl.BlockSpec((count, block), lambda i: (0, i)),
        out_shape=jax.ShapeDtypeStruct((count, features), BF16),
        scratch_shapes=[pltpu.VMEM((count, total), BF16)],
        compiler_params=params(),
        cost_estimate=cost(2 * count * total * features, (count + total) * features * 2),
        name=name,
    )(index.reshape(count, 1), rows)


def hop(value, axis, distance):
    size = lax.axis_size(axis)
    return lax.ppermute(value, axis, [(i, i ^ distance) for i in range(size)])


def piece(stack, index):
    return lax.dynamic_index_in_dim(stack, index, 0, keepdims=False)


def scatter_sum(value, axis, distances, member, carried):
    parts = value.reshape(len(distances), -1, value.shape[-1])
    shift = distances[1].bit_length() - 1
    total = piece(parts, member)
    for distance in distances[1:]:
        sent = piece(parts, member ^ (distance >> shift)).astype(carried)
        total = total + hop(sent, axis, distance).astype(F32)
    return total


def gather_parts(value, axis, distances, member):
    shift = distances[1].bit_length() - 1
    count = len(distances)
    got = [value] + [hop(value, axis, distance) for distance in distances[1:]]
    stack = jnp.zeros((count,) + value.shape, value.dtype)
    for distance, part in zip(distances, got):
        stack = lax.dynamic_update_index_in_dim(stack, part, member ^ (distance >> shift), 0)
    return stack.reshape(-1, value.shape[-1])


def reduction_steps(parts):
    total = jnp.concatenate(parts, axis=0)
    yield total
    seq, rep = lax.axis_index("seq"), lax.axis_index("rep")
    across = list(range(lax.axis_size("seq")))
    along = list(range(0, lax.axis_size("rep"), 2))
    total = scatter_sum(total, "rep", [0, 1], rep % 2, F32)
    yield total
    total = scatter_sum(total, "seq", across, seq, F32)
    yield total
    total = scatter_sum(total, "rep", along, rep // 2, F32).astype(BF16)
    yield total
    total = gather_parts(total, "rep", along, rep // 2)
    yield total
    total = gather_parts(total, "seq", across, seq)
    yield total
    yield gather_parts(total, "rep", [0, 1], rep % 2)


def per_device(tile_embed, tile_source, slide_len, grad_out, w_query, w_key, w_value, w_out):
    owned = tile_embed[0]
    tokens, features = owned.shape
    if tokens != SEG or tokens % RATE:
        raise ValueError("unsupported shard")
    stripes = lax.axis_size("seq")
    stripe = lax.axis_index("seq")
    portion = tokens // stripes
    width = tokens // RATE
    hd = features // HEADS
    scaling = hd ** (-0.5)
    alpha = scaling * LOG2E
    length = slide_len[0]

    place = jnp.arange(tokens)
    order = (place % width) * RATE + place // width
    back = (place % RATE) * width + place // RATE

    mine = tile_source[0].reshape(tokens // LANES, LANES)
    sources = jnp.stack([mine] + [hop(mine, "seq", d) for d in range(1, stripes)])
    sources = sources.reshape(stripes, width, RATE).swapaxes(1, 2).reshape(stripes, tokens)
    owner = sources // tokens
    row = sources % tokens
    hot = owner[:, None, :] == jnp.arange(stripes)[None, :, None]
    earlier = (place[:, None] < place[None, :]).astype(BF16)
    counts = jnp.dot(
        hot.reshape(-1, tokens).astype(BF16), earlier, preferred_element_type=F32
    ).reshape(stripes, stripes, tokens)
    rank = jnp.sum(jnp.where(hot, counts, 0.0), axis=1).astype(jnp.int32)
    asked = jnp.where(owner == stripe, rank, -1)
    slots = jnp.arange(portion)
    wanted = jnp.sum(
        jnp.where(asked[:, None, :] == slots[None, :, None], row[:, None, :], 0), axis=2
    ).reshape(tokens)
    picked = pick(wanted, owned, "pick_send").reshape(stripes, portion, features)
    arrived = jnp.concatenate([picked[0]] + [hop(picked[d], "seq", d) for d in range(1, stripes)])
    slot = (owner[0] ^ stripe) * portion + rank[0]
    x = pick(slot, arrived, "pick_place")

    upstream = pick(order, grad_out[0], "pick_grad")
    positions = stripe * tokens + order
    valid = positions < length
    live = valid.astype(F32)
    gt = (nt(w_out, upstream) * live[None, :]).astype(BF16)

    kt = lax.dot_general(w_key, x, (((0,), (1,)), ((), ())), preferred_element_type=F32).astype(BF16)
    vt = lax.dot_general(w_value, x, (((0,), (1,)), ((), ())), preferred_element_type=F32).astype(BF16)
    qt = lax.dot_general(w_query, x, (((0,), (1,)), ((), ())), preferred_element_type=F32).astype(BF16)

    def own_rows(dense):
        blocks = [
            dense[h * hd : (h + 1) * hd, (h % RATE) * width : (h % RATE + 1) * width]
            for h in range(HEADS)
        ]
        return jnp.concatenate(blocks, axis=0)

    near = jnp.concatenate([own_rows(kt), own_rows(vt)], axis=1)
    far = [near] + [hop(near, "seq", d) for d in range(1, stripes)]
    k2 = jnp.concatenate([part[:, :width] for part in far], axis=1)
    v2 = jnp.concatenate([part[:, width:] for part in far], axis=1)

    lead = jnp.arange(PAD)[:, None] == 0
    bias = jnp.where(lead & ~valid[None, :], NEGATIVE, 0.0).astype(BF16)
    one = jnp.broadcast_to(jnp.where(lead, 1.0, 0.0), (PAD, tokens)).astype(BF16)
    live8 = jnp.broadcast_to(live[None, :], (8, tokens))

    facts = jnp.stack([length, stripe.astype(jnp.int32)])
    osp, lsp, dq2, dk2, dv2 = dilated(
        facts, qt, gt, kt, vt, k2, v2, bias, one, width, alpha, scaling
    )
    shared = [
        jnp.concatenate(
            [dk2[:, d * width : (d + 1) * width], dv2[:, d * width : (d + 1) * width]], axis=1
        )
        for d in range(stripes)
    ]
    shared = sum([hop(shared[d], "seq", d) for d in range(1, stripes)], shared[0])
    dk2 = jnp.concatenate([shared[:, :width]] * (LANES // width), axis=1)
    dv2 = jnp.concatenate([shared[:, width:]] * (LANES // width), axis=1)

    count = HEADS // GROUPS
    blank = jnp.zeros((hd, LANES), F32)
    attended, query_grads, key_grads, value_grads, steps = [], [], [], [], []
    for group in range(GROUPS):
        top = group * count
        settled = group > 0
        outs = ()
        for turn, first in enumerate(range(top, top + count, CALL)):
            if steps and turn in STEP_AT:
                qt = lax.optimization_barrier((qt, next(steps[-1])))[0]
            outs = local(
                top, count, first, CALL, outs, qt, kt, vt, gt, bias, one, live8, osp, lsp, dq2,
                dk2 if settled else blank, dv2 if settled else blank, settled, width, alpha,
                scaling,
            )
        att, dq, dk, dv, ksp, vsp = outs
        if not settled:
            dk, dv = settle(top, dk, dv, ksp, vsp, dk2, dv2, width)
        attended.append(att)
        query_grads.append(dq)
        key_grads.append(dk)
        value_grads.append(dv)
        grads = [lax.dot_general(x, d, (((0,), (1,)), ((), ())), preferred_element_type=F32)
                 for d in (dq, dk, dv)]
        cols = count * hd
        outproj = nn(att, upstream)
        grads += [outproj[:, c : c + cols] for c in range(0, features, cols)]
        steps.append(reduction_steps(grads))
    att = jnp.concatenate(attended, axis=0)
    encoded = (x.astype(F32) + tn(att, w_out)).astype(BF16)
    embed_grad = upstream.astype(F32)
    for grads, weight in ((query_grads, w_query), (key_grads, w_key), (value_grads, w_value)):
        flat = jnp.concatenate(grads, axis=0)
        embed_grad = embed_grad + lax.dot_general(
            flat, weight, (((0,), (1,)), ((), ())), preferred_element_type=F32
        )
    embed_grad = embed_grad.astype(BF16)
    encoded = pick(back, encoded, "pick_encoded")
    embed_grad = pick(back, embed_grad, "pick_embed")
    summed = [list(step)[-1] for step in steps]
    outs = [
        jnp.concatenate([s[i * features : (i + 1) * features] for s in summed], axis=1).astype(F32)
        for i in range(3)
    ]
    last = [
        jnp.concatenate(
            [s[c : c + cols] for c in range(3 * features, 4 * features, cols)], axis=1
        )
        for s in summed
    ]
    outs.append(jnp.concatenate(last, axis=0).astype(F32))
    return (encoded[None], embed_grad[None], outs[0], outs[1], outs[2], outs[3])


def solution(mesh):
    return jax.shard_map(
        per_device,
        mesh=mesh,
        in_specs=(
            P("rep", "seq", None),
            P("rep", "seq"),
            P("rep"),
            P("rep", "seq", None),
            P(),
            P(),
            P(),
            P(),
        ),
        out_specs=(P("rep", "seq", None), P("rep", "seq", None), P(), P(), P(), P()),
        check_vma=False,
    )
```

```python
import functools

import jax
import jax.numpy as jnp
from jax import lax
from jax.experimental import pallas as pl
from jax.experimental.pallas import tpu as pltpu
from jax.sharding import PartitionSpec as P


HEADS = 16
SEG = 1024
RATE = 16
NEGATIVE = -1e30
LOG2E = 1.4426950408889634
SPLIT = (6, 6, 4)
CALL = 2
QB = 512
LANES = 128
PAD = 16
F32 = jnp.float32
BF16 = jnp.bfloat16


def nn(a, b):
    return lax.dot_general(a, b, (((1,), (0,)), ((), ())), preferred_element_type=F32)


def nt(a, b):
    return lax.dot_general(a, b, (((1,), (1,)), ((), ())), preferred_element_type=F32)


def tn(a, b):
    return lax.dot_general(a, b, (((0,), (0,)), ((), ())), preferred_element_type=F32)


def params(grid_rank=1):
    return pltpu.CompilerParams(
        dimension_semantics=("arbitrary",) * grid_rank, vmem_limit_bytes=56 * 1024 * 1024
    )


def cost(flops, size, exps=0):
    return pl.CostEstimate(flops=int(flops), bytes_accessed=int(size), transcendentals=int(exps))


def stack_rows(top, bottom):
    return jnp.concatenate([top, bottom], axis=0)


def dilated_body(width, alpha, scaling, n_ref, q_ref, g_ref, k_ref, v_ref, k2_ref, v2_ref,
                 bias_ref, one_ref, o_ref, lse_ref, dq_ref, dk_ref, dv_ref):
    head = pl.program_id(0)
    tokens = k_ref.shape[1]
    far = k2_ref.shape[1]
    q = q_ref[...]
    g = g_ref[...]
    q_aug = stack_rows(q, one_ref[:, :LANES])
    k_aug = stack_rows(k_ref[...], bias_ref[...])
    s1 = tn(k_aug, q_aug)
    t1 = jnp.max(s1, axis=0, keepdims=True) * alpha
    e1 = jnp.exp2(s1 * alpha - t1)
    l1 = jnp.sum(e1, axis=0, keepdims=True)
    u1 = nn(v_ref[...], e1.astype(BF16))
    k2 = k2_ref[...]
    v2 = v2_ref[...]
    row = lax.broadcasted_iota(jnp.int32, (far, LANES), 0)
    pos = ((row // width) ^ n_ref[1]) * tokens + (row % width) * RATE + head % RATE
    s2 = jnp.where(pos < n_ref[0], tn(k2, q) * alpha, NEGATIVE)
    t2 = jnp.max(s2, axis=0, keepdims=True)
    e2 = jnp.exp2(s2 - t2)
    l2 = jnp.sum(e2, axis=0, keepdims=True)
    u2 = nn(v2, e2.astype(BF16))
    top = jnp.maximum(t1, t2)
    a1 = jnp.exp2(t1 - top)
    a2 = jnp.exp2(t2 - top)
    total = a1 * l1 + a2 * l2
    o = (a1 * u1 + a2 * u2) / total
    lse = top + jnp.log2(total)
    o_ref[...] = o
    lse_ref[0] = jnp.broadcast_to(lse, (8, LANES))
    delta = jnp.sum(g.astype(F32) * o, axis=0, keepdims=True)
    lane = lax.broadcasted_iota(jnp.int32, (1, LANES), 1)
    mine = lane // width == (head % RATE) % (LANES // width)
    keep = jnp.where(mine, 1.0, 0.0)
    p2 = jnp.exp2(s2 - lse) * keep
    ds2 = (p2 * (tn(v2, g) - delta)).astype(BF16)
    dv_ref[...] = nt(g, p2.astype(BF16))
    dq_ref[...] = nn(k2, ds2) * scaling
    dk_ref[...] = nt(q, ds2) * scaling


def dilated(n, qt, gt, kt, vt, k2, v2, bias, one, width, alpha, scaling):
    features, tokens = qt.shape
    hd = features // HEADS
    far = k2.shape[1]
    per = LANES // width
    lanes = lambda h: (h, (h % RATE) // per)
    rows = lambda h: (h, 0)
    fixed = lambda h: (0, 0)
    return pl.pallas_call(
        functools.partial(dilated_body, width, alpha, scaling),
        grid=(HEADS,),
        in_specs=[
            pl.BlockSpec(memory_space=pltpu.SMEM),
            pl.BlockSpec((hd, LANES), lanes),
            pl.BlockSpec((hd, LANES), lanes),
            pl.BlockSpec((hd, tokens), rows),
            pl.BlockSpec((hd, tokens), rows),
            pl.BlockSpec((hd, far), rows),
            pl.BlockSpec((hd, far), rows),
            pl.BlockSpec((PAD, tokens), fixed),
            pl.BlockSpec((PAD, tokens), fixed),
        ],
        out_specs=[
            pl.BlockSpec((hd, LANES), rows),
            pl.BlockSpec((1, 8, LANES), lambda h: (h, 0, 0)),
            pl.BlockSpec((hd, LANES), rows),
            pl.BlockSpec((hd, far), rows),
            pl.BlockSpec((hd, far), rows),
        ],
        out_shape=[
            jax.ShapeDtypeStruct((features, LANES), F32),
            jax.ShapeDtypeStruct((HEADS, 8, LANES), F32),
            jax.ShapeDtypeStruct((features, LANES), F32),
            jax.ShapeDtypeStruct((features, far), F32),
            jax.ShapeDtypeStruct((features, far), F32),
        ],
        compiler_params=params(),
        cost_estimate=cost(HEADS * 8 * tokens * LANES * 64, features * tokens * 6),
        name="dilated",
    )(n, qt, gt, kt, vt, k2, v2, bias, one)


def local_body(first, width, alpha, scaling, settled, kept, *refs):
    (q_ref, k_ref, v_ref, g_ref, bias_ref, one_ref, valid_ref, osp_ref, lsp_ref, dq2_ref,
     dk2_ref, dv2_ref) = refs[:12]
    att_ref, dq_ref, dk_ref, dv_ref, ksp_ref, vsp_ref = refs[12 + kept : 18 + kept]
    e_ref, o_ref, t_ref, lse_ref, p_ref, ds_ref, acc_ref = refs[18 + kept :]
    head = first + pl.program_id(0)
    _, tokens = q_ref.shape
    k_aug = stack_rows(k_ref[...], bias_ref[...])
    for start in range(0, tokens, QB):
        cols = slice(start, start + QB)
        q_aug = stack_rows(q_ref[:, cols], one_ref[:, cols])
        s = tn(k_aug, q_aug)
        t = jnp.max(s, axis=0, keepdims=True) * alpha
        e = jnp.exp2(s * alpha - t)
        total = jnp.sum(e, axis=0, keepdims=True)
        e_ref[:, cols] = e
        u = nn(v_ref[...], e.astype(BF16))
        o_ref[:, cols] = u / total
        t_ref[:, cols] = jnp.broadcast_to(t, (8, QB))
        lse_ref[:, cols] = jnp.broadcast_to(t + jnp.log2(total), (8, QB))
    per = LANES // width
    base = pl.multiple_of(((head % RATE) // per) * LANES, LANES)
    spot = pl.ds(base, LANES)
    lane = lax.broadcasted_iota(jnp.int32, (1, LANES), 1)
    mine = lane // width == (head % RATE) % per
    o_ref[:, spot] = jnp.where(mine, osp_ref[...], o_ref[:, spot])
    lse_ref[:, spot] = jnp.where(mine, lsp_ref[0], lse_ref[:, spot])
    att_ref[...] = (o_ref[...] * valid_ref[0:1, :]).astype(BF16)
    for start in range(0, tokens, QB):
        cols = slice(start, start + QB)
        g = g_ref[:, cols]
        delta = jnp.sum(g.astype(F32) * o_ref[:, cols], axis=0, keepdims=True)
        factor = jnp.exp2(t_ref[0:1, cols] - lse_ref[0:1, cols])
        p = e_ref[:, cols] * factor
        p_ref[:, cols] = p.astype(BF16)
        ds_ref[:, cols] = (p * (tn(v_ref[...], g) - delta)).astype(BF16)
    acc_ref[...] = nn(k_ref[...], ds_ref[...]) * scaling
    acc_ref[:, spot] += dq2_ref[...]
    dq_ref[...] = acc_ref[...].astype(BF16)
    for weights, rows_in, extra, out, special, unit in (
        (ds_ref, q_ref, dk2_ref, dk_ref, ksp_ref, scaling),
        (p_ref, g_ref, dv2_ref, dv_ref, vsp_ref, None),
    ):
        total = nt(weights[...], rows_in[...]).T
        acc_ref[...] = total if unit is None else total * unit
        if settled:
            acc_ref[:, spot] += jnp.where(mine, extra[...], 0.0)
        out[...] = acc_ref[...].astype(BF16)
        special[...] = acc_ref[:, spot]


def local(group, size, first, count, prior, qt, kt, vt, gt, bias, one, valid, osp, lsp, dq2,
          dk2, dv2, settled, width, alpha, scaling):
    features, tokens = qt.shape
    hd = features // HEADS
    rows = lambda h: (h + first, 0)
    mine = lambda h: (h + first - group, 0)
    fixed = lambda h: (0, 0)
    block = pl.BlockSpec((hd, tokens), rows)
    special = pl.BlockSpec((hd, LANES), rows)
    extra = special if settled else pl.BlockSpec((hd, LANES), fixed)
    kept = len(prior)
    return pl.pallas_call(
        functools.partial(local_body, first, width, alpha, scaling, settled, kept),
        grid=(count,),
        in_specs=[
            block, block, block, block,
            pl.BlockSpec((PAD, tokens), fixed),
            pl.BlockSpec((PAD, tokens), fixed),
            pl.BlockSpec((8, tokens), fixed),
            special,
            pl.BlockSpec((1, 8, LANES), lambda h: (h + first, 0, 0)),
            special, extra, extra,
        ] + [pl.BlockSpec(memory_space=pl.ANY)] * kept,
        out_specs=[pl.BlockSpec((hd, tokens), mine)] * 4 + [pl.BlockSpec((hd, LANES), mine)] * 2,
        out_shape=[jax.ShapeDtypeStruct((size * hd, tokens), BF16)] * 4
        + [jax.ShapeDtypeStruct((size * hd, LANES), F32)] * 2,
        scratch_shapes=[
            pltpu.VMEM((tokens, tokens), F32),
            pltpu.VMEM((hd, tokens), F32),
            pltpu.VMEM((8, tokens), F32),
            pltpu.VMEM((8, tokens), F32),
            pltpu.VMEM((tokens, tokens), BF16),
            pltpu.VMEM((tokens, tokens), BF16),
            pltpu.VMEM((hd, tokens), F32),
        ],
        input_output_aliases={12 + i: i for i in range(kept)},
        compiler_params=params(),
        cost_estimate=cost(count * 8 * tokens * tokens * 256, count * hd * tokens * 16),
    )(qt, kt, vt, gt, bias, one, valid, osp, lsp, dq2, dk2, dv2, *prior)


def settle_body(first, width, k_ref, v_ref, dk2_ref, dv2_ref, _, __, k_out, v_out):
    head = first + pl.program_id(0)
    lane = lax.broadcasted_iota(jnp.int32, (1, LANES), 1)
    mine = lane // width == (head % RATE) % (LANES // width)
    k_out[...] = (k_ref[...] + jnp.where(mine, dk2_ref[...], 0.0)).astype(BF16)
    v_out[...] = (v_ref[...] + jnp.where(mine, dv2_ref[...], 0.0)).astype(BF16)


def settle(first, dk, dv, ksp, vsp, dk2, dv2, width):
    rows_all = dk.shape[0]
    hd = dk2.shape[0] // HEADS
    per = LANES // width
    mine = pl.BlockSpec((hd, LANES), lambda h: (h, 0))
    rows = pl.BlockSpec((hd, LANES), lambda h: (h + first, 0))
    spot = pl.BlockSpec((hd, LANES), lambda h: (h, ((h + first) % RATE) // per))
    whole = pl.BlockSpec(memory_space=pl.ANY)
    return pl.pallas_call(
        functools.partial(settle_body, first, width),
        grid=(rows_all // hd,),
        in_specs=[mine, mine, rows, rows, whole, whole],
        out_specs=[spot, spot],
        out_shape=[jax.ShapeDtypeStruct(dk.shape, BF16)] * 2,
        input_output_aliases={4: 0, 5: 1},
        compiler_params=params(),
        cost_estimate=cost(rows_all * LANES * 4, rows_all * LANES * 24),
    )(ksp, vsp, dk2, dv2, dk, dv)


def pick_body(index_ref, rows_ref, out_ref, hot_ref):
    @pl.when(pl.program_id(0) == 0)
    def _():
        which = lax.broadcasted_iota(jnp.int32, hot_ref.shape, 1) == index_ref[...]
        hot_ref[...] = jnp.where(which, 1.0, 0.0).astype(BF16)

    out_ref[...] = nn(hot_ref[...], rows_ref[...]).astype(BF16)


def pick(index, rows):
    total, features = rows.shape
    count = index.shape[0]
    block = 2 * LANES if features % (2 * LANES) == 0 else features
    return pl.pallas_call(
        pick_body,
        grid=(features // block,),
        in_specs=[
            pl.BlockSpec((count, 1), lambda i: (0, 0)),
            pl.BlockSpec((total, block), lambda i: (0, i)),
        ],
        out_specs=pl.BlockSpec((count, block), lambda i: (0, i)),
        out_shape=jax.ShapeDtypeStruct((count, features), BF16),
        scratch_shapes=[pltpu.VMEM((count, total), BF16)],
        compiler_params=params(),
        cost_estimate=cost(2 * count * total * features, (count + total) * features * 2),
    )(index.reshape(count, 1), rows)


def hop(value, axis, distance):
    size = lax.axis_size(axis)
    return lax.ppermute(value, axis, [(i, i ^ distance) for i in range(size)])


def piece(stack, index):
    return lax.dynamic_index_in_dim(stack, index, 0, keepdims=False)


def scatter_sum(value, axis, distances, member, carried):
    parts = value.reshape(len(distances), -1, value.shape[-1])
    shift = distances[1].bit_length() - 1
    total = piece(parts, member)
    for distance in distances[1:]:
        sent = piece(parts, member ^ (distance >> shift)).astype(carried)
        total = total + hop(sent, axis, distance).astype(F32)
    return total


def gather_parts(value, axis, distances, member):
    shift = distances[1].bit_length() - 1
    count = len(distances)
    got = [value] + [hop(value, axis, distance) for distance in distances[1:]]
    stack = jnp.zeros((count,) + value.shape, value.dtype)
    for distance, part in zip(distances, got):
        stack = lax.dynamic_update_index_in_dim(stack, part, member ^ (distance >> shift), 0)
    return stack.reshape(-1, value.shape[-1])


def reduced(parts):
    total = jnp.concatenate(parts, axis=0)
    seq, rep = lax.axis_index("seq"), lax.axis_index("rep")
    across = list(range(lax.axis_size("seq")))
    along = list(range(0, lax.axis_size("rep"), 2))
    total = scatter_sum(total, "rep", [0, 1], rep % 2, F32)
    total = scatter_sum(total, "seq", across, seq, F32)
    total = scatter_sum(total, "rep", along, rep // 2, F32).astype(BF16)
    total = gather_parts(total, "rep", along, rep // 2)
    total = gather_parts(total, "seq", across, seq)
    return gather_parts(total, "rep", [0, 1], rep % 2)


def per_device(tile_embed, tile_source, slide_len, grad_out, w_query, w_key, w_value, w_out):
    owned = tile_embed[0]
    tokens, features = owned.shape
    if tokens != SEG or tokens % RATE:
        raise ValueError("unsupported shard")
    stripes = lax.axis_size("seq")
    stripe = lax.axis_index("seq")
    portion = tokens // stripes
    width = tokens // RATE
    hd = features // HEADS
    scaling = hd ** (-0.5)
    alpha = scaling * LOG2E
    length = slide_len[0]

    place = jnp.arange(tokens)
    order = (place % width) * RATE + place // width
    back = (place % RATE) * width + place // RATE

    mine = tile_source[0].reshape(tokens // LANES, LANES)
    sources = jnp.stack([mine] + [hop(mine, "seq", d) for d in range(1, stripes)])
    sources = sources.reshape(stripes, width, RATE).swapaxes(1, 2).reshape(stripes, tokens)
    owner = sources // tokens
    row = sources % tokens
    hot = owner[:, None, :] == jnp.arange(stripes)[None, :, None]
    earlier = (place[:, None] < place[None, :]).astype(BF16)
    counts = jnp.dot(
        hot.reshape(-1, tokens).astype(BF16), earlier, preferred_element_type=F32
    ).reshape(stripes, stripes, tokens)
    rank = jnp.sum(jnp.where(hot, counts, 0.0), axis=1).astype(jnp.int32)
    asked = jnp.where(owner == stripe, rank, -1)
    slots = jnp.arange(portion)
    wanted = jnp.sum(
        jnp.where(asked[:, None, :] == slots[None, :, None], row[:, None, :], 0), axis=2
    ).reshape(tokens)
    picked = pick(wanted, owned).reshape(stripes, portion, features)
    arrived = jnp.concatenate([picked[0]] + [hop(picked[d], "seq", d) for d in range(1, stripes)])
    slot = (owner[0] ^ stripe) * portion + rank[0]
    x = pick(slot, arrived)

    upstream = pick(order, grad_out[0])
    positions = stripe * tokens + order
    valid = positions < length
    live = valid.astype(F32)
    gt = (nt(w_out, upstream) * live[None, :]).astype(BF16)

    kt = lax.dot_general(w_key, x, (((0,), (1,)), ((), ())), preferred_element_type=F32).astype(BF16)
    vt = lax.dot_general(w_value, x, (((0,), (1,)), ((), ())), preferred_element_type=F32).astype(BF16)
    qt = lax.dot_general(w_query, x, (((0,), (1,)), ((), ())), preferred_element_type=F32).astype(BF16)

    def own_rows(dense):
        blocks = [
            dense[h * hd : (h + 1) * hd, (h % RATE) * width : (h % RATE + 1) * width]
            for h in range(HEADS)
        ]
        return jnp.concatenate(blocks, axis=0)

    near = jnp.concatenate([own_rows(kt), own_rows(vt)], axis=1)
    far = [near] + [hop(near, "seq", d) for d in range(1, stripes)]
    k2 = jnp.concatenate([part[:, :width] for part in far], axis=1)
    v2 = jnp.concatenate([part[:, width:] for part in far], axis=1)

    lead = jnp.arange(PAD)[:, None] == 0
    bias = jnp.where(lead & ~valid[None, :], NEGATIVE, 0.0).astype(BF16)
    one = jnp.broadcast_to(jnp.where(lead, 1.0, 0.0), (PAD, tokens)).astype(BF16)
    live8 = jnp.broadcast_to(live[None, :], (8, tokens))

    facts = jnp.stack([length, stripe.astype(jnp.int32)])
    osp, lsp, dq2, dk2, dv2 = dilated(
        facts, qt, gt, kt, vt, k2, v2, bias, one, width, alpha, scaling
    )
    shared = [
        jnp.concatenate(
            [dk2[:, d * width : (d + 1) * width], dv2[:, d * width : (d + 1) * width]], axis=1
        )
        for d in range(stripes)
    ]
    shared = sum([hop(shared[d], "seq", d) for d in range(1, stripes)], shared[0])
    dk2 = jnp.concatenate([shared[:, :width]] * (LANES // width), axis=1)
    dv2 = jnp.concatenate([shared[:, width:]] * (LANES // width), axis=1)

    blank = jnp.zeros((hd, LANES), F32)
    attended, query_grads, key_grads, value_grads, summed = [], [], [], [], []
    top = 0
    for group, count in enumerate(SPLIT):
        settled = group > 0
        outs = ()
        for first in range(top, top + count, CALL):
            outs = local(
                top, count, first, CALL, outs, qt, kt, vt, gt, bias, one, live8, osp, lsp,
                dq2, dk2 if settled else blank, dv2 if settled else blank, settled, width,
                alpha, scaling,
            )
        att, dq, dk, dv, ksp, vsp = outs
        if not settled:
            dk, dv = settle(top, dk, dv, ksp, vsp, dk2, dv2, width)
        attended.append(att)
        query_grads.append(dq)
        key_grads.append(dk)
        value_grads.append(dv)
        grads = [nn(d, x) for d in (dq, dk, dv)] + [nn(att, upstream)]
        summed.append(reduced(grads))
        top += count
    att = jnp.concatenate(attended, axis=0)
    encoded = (x.astype(F32) + tn(att, w_out)).astype(BF16)
    embed_grad = upstream.astype(F32)
    for grads, weight in ((query_grads, w_query), (key_grads, w_key), (value_grads, w_value)):
        flat = jnp.concatenate(grads, axis=0)
        embed_grad = embed_grad + lax.dot_general(
            flat, weight, (((0,), (1,)), ((), ())), preferred_element_type=F32
        )
    embed_grad = embed_grad.astype(BF16)
    encoded = pick(back, encoded)
    embed_grad = pick(back, embed_grad)
    outs = []
    for kind in range(4):
        rows = [
            part[kind * count * hd : (kind + 1) * count * hd]
            for part, count in zip(summed, SPLIT)
        ]
        whole = jnp.concatenate(rows, axis=0)
        outs.append((whole if kind == 3 else whole.T).astype(F32))
    return (encoded[None], embed_grad[None], outs[0], outs[1], outs[2], outs[3])


def solution(mesh):
    return jax.shard_map(
        per_device,
        mesh=mesh,
        in_specs=(
            P("rep", "seq", None),
            P("rep", "seq"),
            P("rep"),
            P("rep", "seq", None),
            P(),
            P(),
            P(),
            P(),
        ),
        out_specs=(P("rep", "seq", None), P("rep", "seq", None), P(), P(), P(), P()),
        check_vma=False,
    )
```
